32 devices in a mesh: dp: 4 (over x, core), seq: 2 (over y), mp: 4 (over z).
Axes of the slice: x: 2, y: 2, z: 4, core: 2. Of those that a mesh axis runs over, the one named last changes fastest.
Arguments:
- inputs: bfloat16 [6272, 1024], P(('dp', 'seq', 'mp')), may hold values from -6 to 6
- grad_out: bfloat16 [6272, 1024], P(('dp', 'seq', 'mp')), may hold values from -6 to 6
- pad_mask: int32 [6272], P(('dp', 'seq', 'mp')), may hold values from 0 to 1, as said below
- hidden_pre: bfloat16 [6272, 4096], P(('dp', 'seq'), 'mp'), may hold values from -6 to 6
- w_in: bfloat16 [1024, 4096], P(None, 'mp'), may hold values from -0.1875 to 0.1875
- w_out: bfloat16 [4096, 1024], P('mp'), may hold values from -0.09375 to 0.09375
- ln_gain: float32 [1024], replicated, may hold values from 0.25 to 1.75
- ln_shift: float32 [1024], replicated, may hold values from -3 to 3
Outputs:
- grad_inputs: bfloat16 [6272, 1024], P(('dp', 'seq', 'mp'))
- grad_w_in: float32 [1024, 4096], P('seq', 'mp')
- grad_w_out: float32 [4096, 1024], P('mp', 'seq')
The draws below stay inside these ranges and needn't reach their ends.
Inputs may be any that keep to these rules, and one draw needn't show every extreme that they name: `pad_mask`: each window is 196 consecutive tokens, 14 rows of 14 in row order; its image tokens are those in its first h rows and first w columns, h and w between 4 and 14; some windows are full and some are not in every draw.
All inputs are finite; a program needn't handle non-finite values.
Results may differ from the reference program's by a relative error of at most 0.02.
Values may be sent and summed in bfloat16 or wider, within the bound.
A program may use at most 64 MiB of HBM per device.

```python
import jax
import jax.numpy as jnp
from jax import lax

D = 1024
FF = 4096
WT = 196
TOKENS = 6272
N_MP = 4


def draw_pad_mask(key, part):
    windows = TOKENS // WT
    is_full = jax.random.randint(jax.random.fold_in(key, 11), (windows,), 0, 2)
    height = jax.random.randint(jax.random.fold_in(key, 12), (windows,), 4, 15)
    breadth = jax.random.randint(jax.random.fold_in(key, 13), (windows,), 4, 15)
    height = jnp.where(is_full == 1, 14, height)
    breadth = jnp.where(is_full == 1, 14, breadth)
    position = jnp.arange(WT, dtype=jnp.int32)
    row_pos = position // 14
    col_pos = position % 14
    alive_grid = (row_pos[None, :] < height[:, None]) & (col_pos[None, :] < breadth[:, None])
    return alive_grid.astype(jnp.int32).reshape(TOKENS)


def spiked(entries, stream_key, source, target, parts, factor):
    def block_of(axis_at):
        return (jnp.arange(entries.shape[axis_at]) // (entries.shape[axis_at] // parts)).reshape((-1,) + (1,) * (entries.ndim - 1 - axis_at))

    near = jax.random.permutation(stream_key, parts)[block_of(target)]
    second = (block_of(target) + parts // 2) % parts
    return jnp.where((block_of(source) == near) | (block_of(source) == second), factor * entries, entries)


def steps_of(own_key, extent, pieces, smallest, high):
    def one(dim, blocks):
        heights = jax.random.uniform(jax.random.fold_in(jax.random.fold_in(own_key, 6), dim), (blocks,), jnp.float32, smallest / len(pieces), high / len(pieces))
        return jnp.repeat(jnp.exp(heights), extent[dim] // blocks).reshape((-1,) + (1,) * (len(extent) - dim - 1))

    gain = one(*pieces[0])
    for cut in pieces[1:]:
        gain = gain * one(*cut)
    return gain


def scatter_about(own_key, dims, deviation, most, shards=(), held_as=jnp.bfloat16):
    factor_of = steps_of(own_key, dims, shards, -0.22, 0.18) if shards else 1.0
    drawn = jax.random.normal(own_key, dims, jnp.float32) * deviation * factor_of
    return jnp.minimum(jnp.maximum(drawn, -most), most).astype(held_as)


def bell_draw_with(stream_key, shape, deviation, bound, pieces, heavy, held_as=jnp.bfloat16):
    drawn = deviation * jax.random.normal(stream_key, shape, jnp.float32)
    if pieces:
        drawn = drawn * steps_of(stream_key, shape, pieces, -0.22, 0.18)
    return jnp.clip(spiked(drawn, jax.random.fold_in(stream_key, 3), *heavy), -bound, bound).astype(held_as)


def setup_inputs(seed: int = 0) -> dict:
    key_list = jax.random.split(jax.random.key(seed), 9)
    inputs = scatter_about(key_list[0], (TOKENS, D), 1.0, 6.0, ((0, 32),))
    grad_out = bell_draw_with(key_list[1], (TOKENS, D), 1.0, 6.0, ((0, 32),), (0, 1, 32, 2.75))
    pad_mask = draw_pad_mask(jax.random.fold_in(key_list[8], 71), 0)
    hidden_pre = scatter_about(key_list[3], (TOKENS, FF), 1.0, 6.0, ((0, 8), (1, 4)))
    w_in = scatter_about(key_list[4], (D, FF), D ** -0.5, 0.1875, ((1, 4),))
    w_out = scatter_about(key_list[5], (FF, D), FF ** -0.5, 0.09375, ((0, 4),))
    ln_gain = jnp.clip(1.0 + 0.15 * jax.random.normal(key_list[6], (D,), jnp.float32), 0.25, 1.75)
    ln_shift = scatter_about(key_list[7], (D,), 0.5, 3.0, (), jnp.float32)
    return {"inputs": inputs, "grad_out": grad_out, "pad_mask": pad_mask, "hidden_pre": hidden_pre, "w_in": w_in, "w_out": w_out, "ln_gain": ln_gain, "ln_shift": ln_shift}


EPSILON = 1e-06
ROOT_HALF = 0.7071067811865476
INV_ROOT_TAU = 0.3989422804014327

def gelu_pair(hidden_pre):
    values = hidden_pre.astype(jnp.float32)
    normal_cdf = 0.5 * (1.0 + lax.erf(values * ROOT_HALF))
    normal_pdf = jnp.exp(-0.5 * values * values) * INV_ROOT_TAU
    return (values * normal_cdf, normal_cdf + values * normal_pdf)

def layer_norm(inputs, ln_gain, ln_shift):
    values = inputs.astype(jnp.float32)
    row_mean = lax.optimization_barrier(jnp.mean(values, axis=1, keepdims=True))
    centred = values - row_mean
    row_var = lax.optimization_barrier(jnp.mean(centred * centred, axis=1, keepdims=True))
    inv_std = lax.rsqrt(row_var + EPSILON)
    x_hat = centred * inv_std
    normed = (x_hat * ln_gain + ln_shift).astype(jnp.bfloat16)
    return (x_hat, inv_std, normed)

def norm_backward(d_normed, x_hat, inv_std, ln_gain):
    d_hat = d_normed * ln_gain
    first_term = lax.optimization_barrier(jnp.mean(d_hat, axis=1, keepdims=True))
    second_term = lax.optimization_barrier(jnp.mean(d_hat * x_hat, axis=1, keepdims=True))
    return inv_std * (d_hat - first_term - x_hat * second_term)

def reference(inputs, grad_out, pad_mask, hidden_pre, w_in, w_out, ln_gain, ln_shift):
    x_hat, inv_std, normed = layer_norm(inputs, ln_gain, ln_shift)
    masked = (grad_out.astype(jnp.float32) * pad_mask.astype(jnp.float32)[:, None]).astype(jnp.bfloat16)
    activation, slope = gelu_pair(hidden_pre)
    activation = activation.astype(jnp.bfloat16)
    d_act = jnp.dot(masked, w_out.T, preferred_element_type=jnp.float32)
    d_hidden = (d_act * slope).astype(jnp.bfloat16)
    scale = float(TOKENS) ** (-0.5)
    grad_w_out = jnp.dot(activation.T, masked, preferred_element_type=jnp.float32) * scale
    grad_w_in = jnp.dot(normed.T, d_hidden, preferred_element_type=jnp.float32) * scale
    width_block = FF // N_MP
    d_normed = jnp.zeros((inputs.shape[0], D), jnp.float32)
    for shard in range(N_MP):
        left = d_hidden[:, shard * width_block:(shard + 1) * width_block]
        right = w_in[:, shard * width_block:(shard + 1) * width_block]
        partial_sum = jnp.dot(left, right.T, preferred_element_type=jnp.float32)
        partial_sum = lax.optimization_barrier(partial_sum.astype(jnp.bfloat16)).astype(jnp.float32)
        d_normed = d_normed + partial_sum
    grad_inputs = (masked.astype(jnp.float32) + norm_backward(d_normed, x_hat, inv_std, ln_gain)).astype(jnp.bfloat16)
    return (grad_inputs, grad_w_in, grad_w_out)
```

```python
import functools

import jax
import jax.numpy as jnp
from jax import lax
from jax.experimental import pallas as pl
from jax.experimental.pallas import tpu as pltpu
from jax.sharding import PartitionSpec as P

EPSILON = 1e-06
ROOT_HALF = 0.7071067811865476
INV_ROOT_TAU = 0.3989422804014327
MESH = pl.DeviceIdType.MESH
CHUNKS = 2
BF = jnp.bfloat16
F32 = jnp.float32


def kernel(n, x_ref, normed_ref, masked_ref, h_ref, w_in_ref, w_out_ref, gain_ref,
           gi_ref, out_in, out_out,
           m_all, n_all, act, dh, dn, from_left, from_right,
           t_in, t_out, rc_in, rc_out, ry_in, ry_out, rx_in, rx_out,
           m_send, m_recv, n_send, n_recv, r_send, r_recv, d_send, d_recv):
    dp, y, z = lax.axis_index("dp"), lax.axis_index("seq"), lax.axis_index("mp")
    core = lax.rem(dp, 2)
    half = dp // 2
    core_peer = dp + 1 - 2 * core
    x_peer = core + 2 * (1 - half)
    width, ff = w_in_ref.shape
    own_rows = normed_ref.shape[0]

    has = (z < n - 1, z > 0)
    peer = (lax.min(z + 1, n - 1), lax.max(z - 1, 0))

    barrier = pltpu.get_barrier_semaphore()
    for d in (0, 1):
        @pl.when(has[d])
        def _(d=d):
            pl.semaphore_signal(barrier, inc=1, device_id={"mp": peer[d]}, device_id_type=MESH)
    pl.semaphore_signal(barrier, inc=1, device_id={"dp": core_peer}, device_id_type=MESH)
    pl.semaphore_signal(barrier, inc=1, device_id={"dp": x_peer}, device_id_type=MESH)
    pl.semaphore_signal(barrier, inc=1, device_id={"seq": 1 - y}, device_id_type=MESH)
    pl.semaphore_wait(barrier, 3 + jnp.where(z < n - 1, 1, 0) + jnp.where(z > 0, 1, 0))

    def origin(d, s):
        return z - s if d == 0 else z + s

    def arrives(d, s):
        return z >= s if d == 0 else z + s < n

    def gather_copy(own, all_ref, send, recv, d, s):
        t = jnp.clip(origin(d, s), 0, n - 1)
        return pltpu.make_async_remote_copy(
            src_ref=own if s == 0 else all_ref.at[t], dst_ref=all_ref.at[t],
            send_sem=send.at[d, s], recv_sem=recv.at[d, s],
            device_id={"mp": peer[d]}, device_id_type=MESH)

    def landed(all_ref, send, recv, d, s):
        t = jnp.clip(origin(d, s), 0, n - 1)
        return pltpu.make_async_remote_copy(
            src_ref=all_ref.at[t], dst_ref=all_ref.at[t],
            send_sem=send.at[d, s - 1], recv_sem=recv.at[d, s - 1],
            device_id={"mp": peer[d]}, device_id_type=MESH)

    def m_copy(d, s):
        return gather_copy(masked_ref, m_all, m_send, m_recv, d, s)

    def n_copy(d, s):
        return gather_copy(normed_ref, n_all, n_send, n_recv, d, s)

    def forwards(d, s):
        return jnp.logical_and(has[d], arrives(d, s))

    def start_own_normed(s):
        for d, last in ((0, z), (1, n - 1 - z)):
            @pl.when(jnp.logical_and(has[d], last == s))
            def _(d=d):
                n_copy(d, 0).start()

    step = 256

    def process(t):
        def body(c, carry):
            cols = pl.ds(pl.multiple_of(c * step, step), step)
            h = h_ref[t, :, cols].astype(F32)
            cdf = 0.5 * (1.0 + lax.erf(h * ROOT_HALF))
            pdf = jnp.exp(-0.5 * h * h) * INV_ROOT_TAU
            act[t, :, cols] = (h * cdf).astype(BF)
            d_act = lax.dot_general(m_all[t], w_out_ref[cols, :], (((1,), (1,)), ((), ())),
                                    preferred_element_type=F32)
            dh[t, :, cols] = (d_act * (cdf + h * pdf)).astype(BF)
            return carry
        lax.fori_loop(0, ff // step, body, 0)

    for d in (0, 1):
        @pl.when(has[d])
        def _(d=d):
            m_copy(d, 0).start()
    start_own_normed(0)
    m_all[z] = masked_ref[...]
    n_all[z] = normed_ref[...]
    process(z)
    for s in range(1, n):
        for d in (0, 1):
            @pl.when(arrives(d, s))
            def _(d=d):
                landed(m_all, m_send, m_recv, d, s).wait_recv()

            @pl.when(forwards(d, s))
            def _(d=d):
                m_copy(d, s).start()
        start_own_normed(s)
        for d in (0, 1):
            @pl.when(arrives(d, s))
            def _(d=d):
                process(origin(d, s))

    def back(t, carry):
        def body(c, inner):
            cols = pl.ds(pl.multiple_of(c * step, step), step)
            dn[t, :, cols] = lax.dot_general(
                dh[t], w_in_ref[cols, :], (((1,), (1,)), ((), ())),
                preferred_element_type=F32).astype(BF)
            return inner
        return lax.fori_loop(0, width // step, body, carry)
    lax.fori_loop(0, n, back, 0)

    slots = (from_left, from_right)

    def run_copy(d, j):
        t = n - 1 - j if d == 0 else j
        return pltpu.make_async_remote_copy(
            src_ref=dn.at[t], dst_ref=slots[d].at[t],
            send_sem=r_send.at[d, j], recv_sem=r_recv.at[d, j],
            device_id={"mp": peer[d]}, device_id_type=MESH)

    def running(j):
        for d in (0, 1):
            t = n - 1 - j if d == 0 else j
            beyond = z < t if d == 0 else z > t
            gets = jnp.logical_and(has[1 - d], z <= t if d == 0 else z >= t)

            @pl.when(gets)
            def _(d=d, t=t, j=j):
                run_copy(d, j).wait_recv()

            @pl.when(jnp.logical_and(gets, beyond))
            def _(d=d, t=t, j=j):
                dn[t] = (dn[t].astype(F32) + slots[d][t].astype(F32)).astype(BF)

            @pl.when(beyond)
            def _(d=d, t=t, j=j):
                run_copy(d, j).start()

    def grad_parts(which):
        return ((t_in, rc_in, ry_in, rx_in, out_in), (t_out, rc_out, ry_out, rx_out, out_out))[which]

    def d_copy(which, stage, c):
        term, rc, ry, rx, out = grad_parts(which)
        src, dst, target = (
            (term.at[1 - core, c], rc.at[c], {"dp": core_peer}),
            (term.at[core, c, 1 - y], ry.at[c], {"seq": 1 - y}),
            (term.at[core, c, y], rx.at[c], {"dp": x_peer}),
            (out.at[core, c], out.at[core, c], {"dp": core_peer}),
        )[stage]
        return pltpu.make_async_remote_copy(
            src_ref=src, dst_ref=dst, send_sem=d_send.at[which, stage, c],
            recv_sem=d_recv.at[which, stage, c], device_id=target, device_id_type=MESH)

    def tn(lhs, rhs):
        return lax.dot_general(lhs, rhs, (((0,), (0,)), ((), ())), preferred_element_type=F32)

    rows_all = n * own_rows
    r_out, c_out = t_out.shape[3], t_out.shape[4]
    r_in = t_in.shape[3]

    def make_out():
        for c in range(CHUNKS):
            def body(i, carry):
                k = lax.rem(core + 1 + i, 2)
                cols = pl.ds(pl.multiple_of((k * CHUNKS + c) * r_out, r_out), r_out)
                total = tn(act[:, :, cols].reshape(rows_all, r_out),
                           m_all[...].reshape(rows_all, width)).astype(BF)
                for s in range(2):
                    t_out[k, c, s] = total[:, s * c_out:(s + 1) * c_out]
                return carry
            lax.fori_loop(0, 2, body, 0)
            d_copy(1, 0, c).start()

    def make_in():
        for c in range(CHUNKS):
            def body(i, carry):
                k = lax.rem(core + 1 + i // 2, 2)
                s = lax.rem(i, 2)
                cols = pl.ds(pl.multiple_of(((s * 2 + k) * CHUNKS + c) * r_in, r_in), r_in)
                t_in[k, c, s] = tn(n_all[:, :, cols].reshape(rows_all, r_in),
                                   dh[...].reshape(rows_all, ff)).astype(BF)
                return carry
            lax.fori_loop(0, 4, body, 0)
            d_copy(0, 0, c).start()

    def after_core(which):
        term, rc, ry, rx, out = grad_parts(which)
        for c in range(CHUNKS):
            d_copy(which, 0, c).wait_recv()
            for s in (1 - y, y):
                term[core, c, s] = (term[core, c, s].astype(F32) + rc[c, s].astype(F32)).astype(BF)
            d_copy(which, 1, c).start()

    def after_seq(which):
        term, rc, ry, rx, out = grad_parts(which)
        for c in range(CHUNKS):
            d_copy(which, 1, c).wait_recv()
            term[core, c, y] = (term[core, c, y].astype(F32) + ry[c].astype(F32)).astype(BF)
            d_copy(which, 2, c).start()

    def after_chip(which):
        term, rc, ry, rx, out = grad_parts(which)
        for c in range(CHUNKS):
            d_copy(which, 2, c).wait_recv()
            out[core, c] = (term[core, c, y].astype(F32) + rx[c].astype(F32)).astype(BF)
            d_copy(which, 3, c).start()

    stages = [after_core, after_seq, after_chip]
    make_out()
    stages.pop(0)(1)
    for s in range(1, n):
        for d in (0, 1):
            @pl.when(arrives(d, s))
            def _(d=d):
                landed(n_all, n_send, n_recv, d, s).wait_recv()

            @pl.when(forwards(d, s))
            def _(d=d):
                n_copy(d, s).start()
        running(s - 1)
        if stages:
            stages.pop(0)(1)
    for stage in stages:
        stage(1)
    make_in()
    after_core(0)
    running(n - 1)

    def norm_rows(i, carry):
        rows = pl.ds(pl.multiple_of(i * 16, 16), 16)
        values = x_ref[rows, :].astype(F32)
        row_mean = jnp.mean(values, axis=1, keepdims=True)
        centred = values - row_mean
        row_var = jnp.mean(centred * centred, axis=1, keepdims=True)
        inv_std = lax.rsqrt(row_var + EPSILON)
        x_hat = centred * inv_std
        total = dn[z, rows, :].astype(F32)
        left = from_left[z, rows, :].astype(F32)
        right = from_right[z, rows, :].astype(F32)
        total = total + jnp.where(z > 0, left, 0.0) + jnp.where(z < n - 1, right, 0.0)
        d_hat = total * gain_ref[...]
        first = jnp.mean(d_hat, axis=1, keepdims=True)
        second = jnp.mean(d_hat * x_hat, axis=1, keepdims=True)
        gi_ref[rows, :] = (masked_ref[rows, :].astype(F32)
                           + inv_std * (d_hat - first - x_hat * second)).astype(BF)
        return carry

    @pl.when(z == 0)
    def _():
        from_left[z] = jnp.zeros(from_left.shape[1:], BF)

    @pl.when(z == n - 1)
    def _():
        from_right[z] = jnp.zeros(from_right.shape[1:], BF)
    lax.fori_loop(0, own_rows // 16, norm_rows, 0)

    after_seq(0)
    after_chip(0)
    for which in (1, 0):
        for c in range(CHUNKS):
            term, rc, ry, rx, out = grad_parts(which)
            pltpu.make_async_remote_copy(
                src_ref=out.at[1 - core, c], dst_ref=out.at[1 - core, c],
                send_sem=d_send.at[which, 3, c], recv_sem=d_recv.at[which, 3, c],
                device_id={"dp": core_peer}, device_id_type=MESH).wait_recv()
    for which in (1, 0):
        for stage in range(4):
            for c in range(CHUNKS):
                d_copy(which, stage, c).wait_send()
    for s in range(n - 1):
        for d in (0, 1):
            @pl.when(forwards(d, s))
            def _(d=d, s=s):
                m_copy(d, s).wait_send()
                n_copy(d, s).wait_send()
    for j in range(n):
        for d in (0, 1):
            t = n - 1 - j if d == 0 else j

            @pl.when(z < t if d == 0 else z > t)
            def _(d=d, j=j):
                run_copy(d, j).wait_send()


def shards(n, inputs, grad_out, pad_mask, hidden_pre, w_in, w_out, ln_gain, ln_shift):
    own_rows, width = inputs.shape
    ff = w_in.shape[1]
    padded = -(-own_rows // 16) * 16
    grow = ((0, padded - own_rows), (0, 0))
    x = jnp.pad(inputs, grow)
    values = x.astype(F32)
    row_mean = jnp.mean(values, axis=1, keepdims=True)
    centred = values - row_mean
    row_var = jnp.mean(centred * centred, axis=1, keepdims=True)
    inv_std = lax.rsqrt(row_var + EPSILON)
    normed = (centred * inv_std * ln_gain + ln_shift).astype(BF)
    masked = jnp.pad((grad_out.astype(F32) * pad_mask.astype(F32)[:, None]).astype(BF), grow)
    h = jnp.pad(hidden_pre.reshape(n, own_rows, ff), ((0, 0),) + grow)
    in_piece = (width // (4 * CHUNKS), ff)
    out_piece = (ff // (2 * CHUNKS), width // 2)
    block = (n, padded, width)
    scratch = [
        pltpu.VMEM(block, BF), pltpu.VMEM(block, BF),
        pltpu.VMEM((n, padded, ff), BF), pltpu.VMEM((n, padded, ff), BF),
        pltpu.VMEM(block, BF), pltpu.VMEM(block, BF), pltpu.VMEM(block, BF),
    ]
    scratch += [pltpu.VMEM((2, CHUNKS, 2) + p, BF) for p in (in_piece, out_piece)]
    scratch += [pltpu.VMEM((CHUNKS, 2) + p, BF) for p in (in_piece, out_piece)]
    scratch += [pltpu.VMEM((CHUNKS,) + p, BF) for p in (in_piece, out_piece)] * 2
    scratch += [pltpu.SemaphoreType.DMA((2, n))] * 6
    scratch += [pltpu.SemaphoreType.DMA((2, 4, CHUNKS))] * 2
    vmem = pl.BlockSpec(memory_space=pltpu.VMEM)
    gi, g_in, g_out = pl.pallas_call(
        functools.partial(kernel, n),
        out_shape=(
            jax.ShapeDtypeStruct((padded, width), BF),
            jax.ShapeDtypeStruct((2, CHUNKS) + in_piece, BF),
            jax.ShapeDtypeStruct((2, CHUNKS) + out_piece, BF),
        ),
        in_specs=[vmem] * 7,
        out_specs=(vmem,) * 3,
        scratch_shapes=scratch,
        name="mlp_backward",
        compiler_params=pltpu.CompilerParams(
            collective_id=0, has_side_effects=True, vmem_limit_bytes=60 * 1024 * 1024),
    )(x, normed, masked, h, w_in, w_out, ln_gain.reshape(1, width))
    token_total = own_rows * lax.axis_size("dp") * lax.axis_size("seq") * n
    scale = float(token_total) ** (-0.5)
    return (
        gi[:own_rows],
        g_in.reshape(width // 2, ff).astype(F32) * scale,
        g_out.reshape(ff, width // 2).astype(F32) * scale,
    )


def gelu_pair(hidden_pre):
    values = hidden_pre.astype(jnp.float32)
    normal_cdf = 0.5 * (1.0 + lax.erf(values * ROOT_HALF))
    normal_pdf = jnp.exp(-0.5 * values * values) * INV_ROOT_TAU
    return (values * normal_cdf, normal_cdf + values * normal_pdf)


def plain_shards(inputs, grad_out, pad_mask, hidden_pre, w_in, w_out, ln_gain, ln_shift):
    own_rows = inputs.shape[0]
    values = inputs.astype(jnp.float32)
    row_mean = jnp.mean(values, axis=1, keepdims=True)
    centred = values - row_mean
    row_var = jnp.mean(centred * centred, axis=1, keepdims=True)
    inv_std = lax.rsqrt(row_var + EPSILON)
    x_hat = centred * inv_std
    normed = (x_hat * ln_gain + ln_shift).astype(jnp.bfloat16)
    masked = (grad_out.astype(jnp.float32) * pad_mask.astype(jnp.float32)[:, None]).astype(
        jnp.bfloat16
    )
    normed_all, masked_all = (
        lax.all_gather(normed, "mp", axis=0, tiled=True),
        lax.all_gather(masked, "mp", axis=0, tiled=True),
    )
    activation, slope = gelu_pair(hidden_pre)
    activation = activation.astype(jnp.bfloat16)
    d_act = jnp.dot(masked_all, w_out.T, preferred_element_type=jnp.float32)
    d_hidden = (d_act * slope).astype(jnp.bfloat16)
    term_out = jnp.dot(activation.T, masked_all, preferred_element_type=jnp.float32)
    term_in = jnp.dot(normed_all.T, d_hidden, preferred_element_type=jnp.float32)
    d_normed = lax.psum_scatter(
        jnp.dot(d_hidden, w_in.T, preferred_element_type=jnp.float32).astype(jnp.bfloat16),
        "mp",
        scatter_dimension=0,
        tiled=True,
    ).astype(jnp.float32)
    d_hat = d_normed * ln_gain
    first_term = jnp.mean(d_hat, axis=1, keepdims=True)
    second_term = jnp.mean(d_hat * x_hat, axis=1, keepdims=True)
    grad_inputs = (
        masked.astype(jnp.float32) + inv_std * (d_hat - first_term - x_hat * second_term)
    ).astype(jnp.bfloat16)
    piece_in, piece_out = (
        lax.psum_scatter(
            term_in.astype(jnp.bfloat16), "seq", scatter_dimension=0, tiled=True
        ).astype(jnp.float32),
        lax.psum_scatter(
            term_out.astype(jnp.bfloat16), "seq", scatter_dimension=1, tiled=True
        ).astype(jnp.float32),
    )
    piece_in, piece_out = (
        lax.psum(piece_in.astype(jnp.bfloat16), "dp").astype(jnp.float32),
        lax.psum(piece_out.astype(jnp.bfloat16), "dp").astype(jnp.float32),
    )
    token_total = own_rows * lax.axis_size("dp") * lax.axis_size("seq") * lax.axis_size("mp")
    scale = float(token_total) ** (-0.5)
    return (grad_inputs, piece_in * scale, piece_out * scale)


def solution(mesh):
    n = mesh.shape["mp"]
    paired = mesh.shape["seq"] == 2 and mesh.shape["dp"] == 4
    return jax.shard_map(
        functools.partial(shards, n) if paired else plain_shards,
        mesh=mesh,
        in_specs=(
            P(("dp", "seq", "mp"), None),
            P(("dp", "seq", "mp"), None),
            P(("dp", "seq", "mp")),
            P(("dp", "seq"), "mp"),
            P(None, "mp"),
            P("mp", None),
            P(),
            P(),
        ),
        out_specs=(P(("dp", "seq", "mp"), None), P("seq", "mp"), P("mp", "seq")),
        check_vma=False,
    )
```

```python
import functools

import jax
import jax.numpy as jnp
from jax import lax
from jax.experimental import pallas as pl
from jax.experimental.pallas import tpu as pltpu
from jax.sharding import PartitionSpec as P

EPSILON = 1e-06
ROOT_HALF = 0.7071067811865476
INV_ROOT_TAU = 0.3989422804014327
MESH = pl.DeviceIdType.MESH
CHUNKS = 2
BF = jnp.bfloat16
F32 = jnp.float32


def kernel(n, x_ref, normed_ref, masked_ref, h_ref, w_in_ref, w_out_ref, gain_ref,
           gi_ref, out_in, out_out,
           m_all, n_all, act, dh, dn, from_left, from_right,
           t_in, t_out, rc_in, rc_out, ry_in, ry_out, rx_in, rx_out,
           m_send, m_recv, n_send, n_recv, r_send, r_recv, d_send, d_recv):
    dp, y, z = lax.axis_index("dp"), lax.axis_index("seq"), lax.axis_index("mp")
    core = lax.rem(dp, 2)
    half = dp // 2
    core_peer = dp + 1 - 2 * core
    x_peer = core + 2 * (1 - half)
    width, ff = w_in_ref.shape
    own_rows = normed_ref.shape[0]

    has = (z < n - 1, z > 0)
    peer = (lax.min(z + 1, n - 1), lax.max(z - 1, 0))

    barrier = pltpu.get_barrier_semaphore()
    for d in (0, 1):
        @pl.when(has[d])
        def _(d=d):
            pl.semaphore_signal(barrier, inc=1, device_id={"mp": peer[d]}, device_id_type=MESH)
    pl.semaphore_signal(barrier, inc=1, device_id={"dp": core_peer}, device_id_type=MESH)
    pl.semaphore_signal(barrier, inc=1, device_id={"dp": x_peer}, device_id_type=MESH)
    pl.semaphore_signal(barrier, inc=1, device_id={"seq": 1 - y}, device_id_type=MESH)
    pl.semaphore_wait(barrier, 3 + jnp.where(z < n - 1, 1, 0) + jnp.where(z > 0, 1, 0))

    def origin(d, s):
        return z - s if d == 0 else z + s

    def arrives(d, s):
        return z >= s if d == 0 else z + s < n

    def gather_copy(own, all_ref, send, recv, d, s):
        t = jnp.clip(origin(d, s), 0, n - 1)
        return pltpu.make_async_remote_copy(
            src_ref=own if s == 0 else all_ref.at[t], dst_ref=all_ref.at[t],
            send_sem=send.at[d, s], recv_sem=recv.at[d, s],
            device_id={"mp": peer[d]}, device_id_type=MESH)

    def landed(all_ref, send, recv, d, s):
        t = jnp.clip(origin(d, s), 0, n - 1)
        return pltpu.make_async_remote_copy(
            src_ref=all_ref.at[t], dst_ref=all_ref.at[t],
            send_sem=send.at[d, s - 1], recv_sem=recv.at[d, s - 1],
            device_id={"mp": peer[d]}, device_id_type=MESH)

    def m_copy(d, s):
        return gather_copy(masked_ref, m_all, m_send, m_recv, d, s)

    def n_copy(d, s):
        return gather_copy(normed_ref, n_all, n_send, n_recv, d, s)

    def forwards(d, s):
        return jnp.logical_and(has[d], arrives(d, s))

    def start_own_normed(s):
        for d, last in ((0, z), (1, n - 1 - z)):
            @pl.when(jnp.logical_and(has[d], last == s))
            def _(d=d):
                n_copy(d, 0).start()

    step = 256

    def process(t):
        def body(c, carry):
            cols = pl.ds(pl.multiple_of(c * step, step), step)
            h = h_ref[t, :, cols].astype(F32)
            cdf = 0.5 * (1.0 + lax.erf(h * ROOT_HALF))
            pdf = jnp.exp(-0.5 * h * h) * INV_ROOT_TAU
            act[t, :, cols] = (h * cdf).astype(BF)
            d_act = lax.dot_general(m_all[t], w_out_ref[cols, :], (((1,), (1,)), ((), ())),
                                    preferred_element_type=F32)
            dh[t, :, cols] = (d_act * (cdf + h * pdf)).astype(BF)
            return carry
        lax.fori_loop(0, ff // step, body, 0)

    for d in (0, 1):
        @pl.when(has[d])
        def _(d=d):
            m_copy(d, 0).start()
    start_own_normed(0)
    m_all[z] = masked_ref[...]
    n_all[z] = normed_ref[...]
    process(z)
    for s in range(1, n):
        for d in (0, 1):
            @pl.when(arrives(d, s))
            def _(d=d):
                landed(m_all, m_send, m_recv, d, s).wait_recv()

            @pl.when(forwards(d, s))
            def _(d=d):
                m_copy(d, s).start()
        start_own_normed(s)
        for d in (0, 1):
            @pl.when(arrives(d, s))
            def _(d=d):
                process(origin(d, s))

    def back(t, carry):
        def body(c, inner):
            cols = pl.ds(pl.multiple_of(c * step, step), step)
            dn[t, :, cols] = lax.dot_general(
                dh[t], w_in_ref[cols, :], (((1,), (1,)), ((), ())),
                preferred_element_type=F32).astype(BF)
            return inner
        return lax.fori_loop(0, width // step, body, carry)
    lax.fori_loop(0, n, back, 0)

    slots = (from_left, from_right)

    def run_copy(d, j):
        t = n - 1 - j if d == 0 else j
        return pltpu.make_async_remote_copy(
            src_ref=dn.at[t], dst_ref=slots[d].at[t],
            send_sem=r_send.at[d, j], recv_sem=r_recv.at[d, j],
            device_id={"mp": peer[d]}, device_id_type=MESH)

    def line_step(d, k):
        return k - z if d == 0 else k - (n - 1 - z)

    def running(k):
        for d in (0, 1):
            j = line_step(d, k)
            t = n - 1 - j if d == 0 else j
            gets = jnp.logical_and(has[1 - d], j >= 0)

            @pl.when(gets)
            def _(d=d, t=t, j=j):
                run_copy(d, j).wait_recv()
                if k < n - 1:
                    dn[t] = (dn[t].astype(F32) + slots[d][t].astype(F32)).astype(BF)

            if k < n - 1:
                @pl.when(j >= 0)
                def _(d=d, j=j):
                    run_copy(d, j).start()

    def grad_parts(which):
        return ((t_in, rc_in, ry_in, rx_in, out_in), (t_out, rc_out, ry_out, rx_out, out_out))[which]

    def d_copy(which, stage, c):
        term, rc, ry, rx, out = grad_parts(which)
        src, dst, target = (
            (term.at[1 - core, c], rc.at[c], {"dp": core_peer}),
            (term.at[core, c, 1 - y], ry.at[c], {"seq": 1 - y}),
            (term.at[core, c, y], rx.at[c], {"dp": x_peer}),
            (out.at[core, c], out.at[core, c], {"dp": core_peer}),
        )[stage]
        return pltpu.make_async_remote_copy(
            src_ref=src, dst_ref=dst, send_sem=d_send.at[which, stage, c],
            recv_sem=d_recv.at[which, stage, c], device_id=target, device_id_type=MESH)

    def tn(lhs, rhs):
        return lax.dot_general(lhs, rhs, (((0,), (0,)), ((), ())), preferred_element_type=F32)

    rows_all = n * own_rows
    r_out, c_out = t_out.shape[3], t_out.shape[4]
    r_in = t_in.shape[3]

    def make_out():
        for c in range(CHUNKS):
            def body(i, carry):
                k = lax.rem(core + 1 + i, 2)
                cols = pl.ds(pl.multiple_of((k * CHUNKS + c) * r_out, r_out), r_out)
                total = tn(act[:, :, cols].reshape(rows_all, r_out),
                           m_all[...].reshape(rows_all, width)).astype(BF)
                for s in range(2):
                    t_out[k, c, s] = total[:, s * c_out:(s + 1) * c_out]
                return carry
            lax.fori_loop(0, 2, body, 0)
            d_copy(1, 0, c).start()

    def make_in():
        for c in range(CHUNKS):
            def body(i, carry):
                k = lax.rem(core + 1 + i // 2, 2)
                s = lax.rem(i, 2)
                cols = pl.ds(pl.multiple_of(((s * 2 + k) * CHUNKS + c) * r_in, r_in), r_in)
                t_in[k, c, s] = tn(n_all[:, :, cols].reshape(rows_all, r_in),
                                   dh[...].reshape(rows_all, ff)).astype(BF)
                return carry
            lax.fori_loop(0, 4, body, 0)
            d_copy(0, 0, c).start()

    def after_core(which):
        term, rc, ry, rx, out = grad_parts(which)
        for c in range(CHUNKS):
            d_copy(which, 0, c).wait_recv()
            for s in (1 - y, y):
                term[core, c, s] = (term[core, c, s].astype(F32) + rc[c, s].astype(F32)).astype(BF)
            d_copy(which, 1, c).start()

    def after_seq(which):
        term, rc, ry, rx, out = grad_parts(which)
        for c in range(CHUNKS):
            d_copy(which, 1, c).wait_recv()
            term[core, c, y] = (term[core, c, y].astype(F32) + ry[c].astype(F32)).astype(BF)
            d_copy(which, 2, c).start()

    def after_chip(which):
        term, rc, ry, rx, out = grad_parts(which)
        for c in range(CHUNKS):
            d_copy(which, 2, c).wait_recv()
            out[core, c] = (term[core, c, y].astype(F32) + rx[c].astype(F32)).astype(BF)
            d_copy(which, 3, c).start()

    stages = [after_core, after_seq, after_chip]
    running(0)
    make_out()
    stages.pop(0)(1)
    for s in range(1, n):
        for d in (0, 1):
            @pl.when(arrives(d, s))
            def _(d=d):
                landed(n_all, n_send, n_recv, d, s).wait_recv()

            @pl.when(forwards(d, s))
            def _(d=d):
                n_copy(d, s).start()
        if s < n - 1:
            running(s)
        if stages:
            stages.pop(0)(1)
    for stage in stages:
        stage(1)
    make_in()
    after_core(0)
    running(n - 1)

    def norm_rows(i, carry):
        rows = pl.ds(pl.multiple_of(i * 16, 16), 16)
        values = x_ref[rows, :].astype(F32)
        row_mean = jnp.mean(values, axis=1, keepdims=True)
        centred = values - row_mean
        row_var = jnp.mean(centred * centred, axis=1, keepdims=True)
        inv_std = lax.rsqrt(row_var + EPSILON)
        x_hat = centred * inv_std
        total = dn[z, rows, :].astype(F32)
        left = from_left[z, rows, :].astype(F32)
        right = from_right[z, rows, :].astype(F32)
        total = total + jnp.where(z > 0, left, 0.0) + jnp.where(z < n - 1, right, 0.0)
        d_hat = total * gain_ref[...]
        first = jnp.mean(d_hat, axis=1, keepdims=True)
        second = jnp.mean(d_hat * x_hat, axis=1, keepdims=True)
        gi_ref[rows, :] = (masked_ref[rows, :].astype(F32)
                           + inv_std * (d_hat - first - x_hat * second)).astype(BF)
        return carry

    @pl.when(z == 0)
    def _():
        from_left[z] = jnp.zeros(from_left.shape[1:], BF)

    @pl.when(z == n - 1)
    def _():
        from_right[z] = jnp.zeros(from_right.shape[1:], BF)
    lax.fori_loop(0, own_rows // 16, norm_rows, 0)

    after_seq(0)
    after_chip(0)
    for which in (1, 0):
        for c in range(CHUNKS):
            term, rc, ry, rx, out = grad_parts(which)
            pltpu.make_async_remote_copy(
                src_ref=out.at[1 - core, c], dst_ref=out.at[1 - core, c],
                send_sem=d_send.at[which, 3, c], recv_sem=d_recv.at[which, 3, c],
                device_id={"dp": core_peer}, device_id_type=MESH).wait_recv()
    for which in (1, 0):
        for stage in range(4):
            for c in range(CHUNKS):
                d_copy(which, stage, c).wait_send()
    for s in range(n - 1):
        for d in (0, 1):
            @pl.when(forwards(d, s))
            def _(d=d, s=s):
                m_copy(d, s).wait_send()
                n_copy(d, s).wait_send()
    for k in range(n - 1):
        for d in (0, 1):
            j = line_step(d, k)

            @pl.when(j >= 0)
            def _(d=d, j=j):
                run_copy(d, j).wait_send()


def shards(n, inputs, grad_out, pad_mask, hidden_pre, w_in, w_out, ln_gain, ln_shift):
    own_rows, width = inputs.shape
    ff = w_in.shape[1]
    padded = -(-own_rows // 16) * 16
    grow = ((0, padded - own_rows), (0, 0))
    x = jnp.pad(inputs, grow)
    values = x.astype(F32)
    row_mean = jnp.mean(values, axis=1, keepdims=True)
    centred = values - row_mean
    row_var = jnp.mean(centred * centred, axis=1, keepdims=True)
    inv_std = lax.rsqrt(row_var + EPSILON)
    normed = (centred * inv_std * ln_gain + ln_shift).astype(BF)
    masked = jnp.pad((grad_out.astype(F32) * pad_mask.astype(F32)[:, None]).astype(BF), grow)
    h = jnp.pad(hidden_pre.reshape(n, own_rows, ff), ((0, 0),) + grow)
    in_piece = (width // (4 * CHUNKS), ff)
    out_piece = (ff // (2 * CHUNKS), width // 2)
    block = (n, padded, width)
    scratch = [
        pltpu.VMEM(block, BF), pltpu.VMEM(block, BF),
        pltpu.VMEM((n, padded, ff), BF), pltpu.VMEM((n, padded, ff), BF),
        pltpu.VMEM(block, BF), pltpu.VMEM(block, BF), pltpu.VMEM(block, BF),
    ]
    scratch += [pltpu.VMEM((2, CHUNKS, 2) + p, BF) for p in (in_piece, out_piece)]
    scratch += [pltpu.VMEM((CHUNKS, 2) + p, BF) for p in (in_piece, out_piece)]
    scratch += [pltpu.VMEM((CHUNKS,) + p, BF) for p in (in_piece, out_piece)] * 2
    scratch += [pltpu.SemaphoreType.DMA((2, n))] * 6
    scratch += [pltpu.SemaphoreType.DMA((2, 4, CHUNKS))] * 2
    vmem = pl.BlockSpec(memory_space=pltpu.VMEM)
    gi, g_in, g_out = pl.pallas_call(
        functools.partial(kernel, n),
        out_shape=(
            jax.ShapeDtypeStruct((padded, width), BF),
            jax.ShapeDtypeStruct((2, CHUNKS) + in_piece, BF),
            jax.ShapeDtypeStruct((2, CHUNKS) + out_piece, BF),
        ),
        in_specs=[vmem] * 7,
        out_specs=(vmem,) * 3,
        scratch_shapes=scratch,
        name="mlp_backward",
        compiler_params=pltpu.CompilerParams(
            collective_id=0, has_side_effects=True, vmem_limit_bytes=60 * 1024 * 1024),
    )(x, normed, masked, h, w_in, w_out, ln_gain.reshape(1, width))
    token_total = own_rows * lax.axis_size("dp") * lax.axis_size("seq") * n
    scale = float(token_total) ** (-0.5)
    return (
        gi[:own_rows],
        g_in.reshape(width // 2, ff).astype(F32) * scale,
        g_out.reshape(ff, width // 2).astype(F32) * scale,
    )


def gelu_pair(hidden_pre):
    values = hidden_pre.astype(jnp.float32)
    normal_cdf = 0.5 * (1.0 + lax.erf(values * ROOT_HALF))
    normal_pdf = jnp.exp(-0.5 * values * values) * INV_ROOT_TAU
    return (values * normal_cdf, normal_cdf + values * normal_pdf)


def plain_shards(inputs, grad_out, pad_mask, hidden_pre, w_in, w_out, ln_gain, ln_shift):
    own_rows = inputs.shape[0]
    values = inputs.astype(jnp.float32)
    row_mean = jnp.mean(values, axis=1, keepdims=True)
    centred = values - row_mean
    row_var = jnp.mean(centred * centred, axis=1, keepdims=True)
    inv_std = lax.rsqrt(row_var + EPSILON)
    x_hat = centred * inv_std
    normed = (x_hat * ln_gain + ln_shift).astype(jnp.bfloat16)
    masked = (grad_out.astype(jnp.float32) * pad_mask.astype(jnp.float32)[:, None]).astype(
        jnp.bfloat16
    )
    normed_all, masked_all = (
        lax.all_gather(normed, "mp", axis=0, tiled=True),
        lax.all_gather(masked, "mp", axis=0, tiled=True),
    )
    activation, slope = gelu_pair(hidden_pre)
    activation = activation.astype(jnp.bfloat16)
    d_act = jnp.dot(masked_all, w_out.T, preferred_element_type=jnp.float32)
    d_hidden = (d_act * slope).astype(jnp.bfloat16)
    term_out = jnp.dot(activation.T, masked_all, preferred_element_type=jnp.float32)
    term_in = jnp.dot(normed_all.T, d_hidden, preferred_element_type=jnp.float32)
    d_normed = lax.psum_scatter(
        jnp.dot(d_hidden, w_in.T, preferred_element_type=jnp.float32).astype(jnp.bfloat16),
        "mp",
        scatter_dimension=0,
        tiled=True,
    ).astype(jnp.float32)
    d_hat = d_normed * ln_gain
    first_term = jnp.mean(d_hat, axis=1, keepdims=True)
    second_term = jnp.mean(d_hat * x_hat, axis=1, keepdims=True)
    grad_inputs = (
        masked.astype(jnp.float32) + inv_std * (d_hat - first_term - x_hat * second_term)
    ).astype(jnp.bfloat16)
    piece_in, piece_out = (
        lax.psum_scatter(
            term_in.astype(jnp.bfloat16), "seq", scatter_dimension=0, tiled=True
        ).astype(jnp.float32),
        lax.psum_scatter(
            term_out.astype(jnp.bfloat16), "seq", scatter_dimension=1, tiled=True
        ).astype(jnp.float32),
    )
    piece_in, piece_out = (
        lax.psum(piece_in.astype(jnp.bfloat16), "dp").astype(jnp.float32),
        lax.psum(piece_out.astype(jnp.bfloat16), "dp").astype(jnp.float32),
    )
    token_total = own_rows * lax.axis_size("dp") * lax.axis_size("seq") * lax.axis_size("mp")
    scale = float(token_total) ** (-0.5)
    return (grad_inputs, piece_in * scale, piece_out * scale)


def solution(mesh):
    n = mesh.shape["mp"]
    paired = mesh.shape["seq"] == 2 and mesh.shape["dp"] == 4
    return jax.shard_map(
        functools.partial(shards, n) if paired else plain_shards,
        mesh=mesh,
        in_specs=(
            P(("dp", "seq", "mp"), None),
            P(("dp", "seq", "mp"), None),
            P(("dp", "seq", "mp")),
            P(("dp", "seq"), "mp"),
            P(None, "mp"),
            P("mp", None),
            P(),
            P(),
        ),
        out_specs=(P(("dp", "seq", "mp"), None), P("seq", "mp"), P("mp", "seq")),
        check_vma=False,
    )
```
